256 devices in a mesh: groups: 2 (over y), blk: 128 (over z, x, core).
Axes of the slice: x: 4, y: 2, z: 16, core: 2. Of those that a mesh axis runs over, the one named last changes fastest.
The devices are a block of a 4x16x16 slice.
Arguments:
- basis: float32 [8, 512, 480, 128], P(None, ('groups', 'blk')), parts along dimension 1
- nbr_block: int32 [512, 14], P(('groups', 'blk')), parts along dimension 0, may hold values from 0 to 255, as said below
- nbr_type: int32 [512, 14], P(('groups', 'blk')), parts along dimension 0, may hold values from 0 to 7
- nbr_count: int32 [512], P(('groups', 'blk')), parts along dimension 0, may hold values from 2 to 14, as said below
- sphere_type: int32 [512, 128], P(('groups', 'blk')), parts along dimension 0, may hold values from 0 to 3
- trans: float32 [8, 480, 480], replicated, may hold values from -0.25 to 0.25
- coup: float32 [8, 128, 128], replicated, may hold values from -0.5 to 0.5
- tmat: float32 [4, 480, 480], replicated, may hold values from -0.125 to 0.125
Outputs:
- new_vectors: float32 [2, 512, 480, 128], P(None, ('groups', 'blk')), parts along dimension 1
- hess_first: float32 [18], P('groups'), parts along dimension 0
- hess_second: float32 [20], P('groups'), parts along dimension 0
The draws below stay inside these ranges and needn't reach their ends.
There are 2 independent parts, one for each index of `groups`. The reference program is written for one: setup_inputs(seed, part) draws one part's arguments, and reference() takes and returns one part's arrays. A program takes and returns all parts, laid end to end along the dimension named above; an argument that names none is the same for every part. Nothing has to cross between parts.
Inputs may be any that keep to these rules, and one draw needn't show every extreme that they name: `nbr_block`: each entry lies within 2 blocks of its own block; a block may be near itself. The first two slots of block b hold, in either order, the blocks b - 2 and b + 2, clipped to the cluster. Block b uses the first nbr_count[b] slots of its lists; some run of blocks uses all 14.
All inputs are finite; a program needn't handle non-finite values.
Results may differ from the reference program's by a relative error of at most 0.0003.
Values sent between devices are 32-bit elements; how exact they have to be, the bound alone decides.
A program may use at most 128 MiB of HBM per device.

```python
import jax
import jax.numpy as jnp
from jax import lax

COEF = 480
SPB = 128
BLK_DEV = 2
NBR = 14
NTYPE = 8
NSTYPE = 4
KRY = 8
RADIUS = 2
NBLOCKS = 256


def draw_basis(key, part):
    common = jax.random.normal(jax.random.fold_in(key, 1), (NBLOCKS, COEF, SPB), jnp.float32)
    strength = jax.random.uniform(jax.random.fold_in(key, 2), (KRY,), jnp.float32, 0.5, 1.0)
    position = jnp.arange(NBLOCKS, dtype=jnp.float32) / float(max(NBLOCKS - 1, 1))
    rough_part = jax.random.normal(jax.random.fold_in(key, 3), (KRY, NBLOCKS, COEF, SPB), jnp.float32)
    ramp_scale = 0.5 + position
    return strength[:, None, None, None] * ramp_scale[None, :, None, None] * common[None] + rough_part


def draw_nbr_block(key, part):
    offsets = jax.random.randint(jax.random.fold_in(key, 11), (NBLOCKS, NBR), -RADIUS, RADIUS + 1)
    flipped = jax.random.randint(jax.random.fold_in(key, 12), (NBLOCKS,), 0, 2)
    lower_first = jnp.where(flipped == 0, -RADIUS, RADIUS)
    slot_index = jnp.arange(NBR, dtype=jnp.int32)[None, :]
    offsets = jnp.where(slot_index == 0, lower_first[:, None], offsets)
    offsets = jnp.where(slot_index == 1, -lower_first[:, None], offsets)
    base_rows = jnp.arange(NBLOCKS, dtype=jnp.int32)[:, None]
    return jnp.clip(base_rows + offsets, 0, NBLOCKS - 1).astype(jnp.int32)


def draw_nbr_count(key, part):
    center = jax.random.randint(jax.random.fold_in(key, 21), (), 0, NBLOCKS)
    light_count = jax.random.randint(jax.random.fold_in(key, 22), (NBLOCKS,), 2, NBR // 2 + 2)
    light_count = jnp.minimum(light_count, NBR)
    block_rows = jnp.arange(NBLOCKS, dtype=jnp.int32)
    dense_run = jnp.abs(block_rows - center) < 2 * BLK_DEV
    return jnp.where(dense_run, NBR, light_count).astype(jnp.int32)


def set_ends(drawn, rng, low, high):
    longest = drawn.shape.index(max(drawn.shape))
    spots = []
    for shift in (0, 1):
        where = [jax.random.randint(jax.random.fold_in(rng, axis), (), 0, length) for axis, length in enumerate(drawn.shape)]
        where[longest] = (where[longest] + shift) % drawn.shape[longest]
        spots.append(tuple(where))
    return drawn.at[spots[0]].set(low).at[spots[1]].set(high)


def scatter_about(stream_key, shape, spread, reach, held_as=jnp.bfloat16):
    array = jax.random.normal(stream_key, shape, jnp.float32) * spread
    return jnp.minimum(jnp.maximum(array, -reach), reach).astype(held_as)


def setup_inputs(seed: int = 0, part: int = 0) -> dict:
    streams_of = jax.random.split(jax.random.key(seed), 9)
    own_keys = jax.random.split(jax.random.fold_in(streams_of[8], part), 9)
    return {
        "basis": draw_basis(jax.random.fold_in(jax.random.fold_in(streams_of[8], part), 71), part),
        "nbr_block": draw_nbr_block(jax.random.fold_in(jax.random.fold_in(streams_of[8], part), 71), part),
        "nbr_type": set_ends(jax.random.randint(own_keys[2], (NBLOCKS, NBR), 0, NTYPE), jax.random.fold_in(own_keys[2], 1), 0, NTYPE - 1).astype(jnp.int32),
        "nbr_count": draw_nbr_count(jax.random.fold_in(jax.random.fold_in(streams_of[8], part), 71), part),
        "sphere_type": set_ends(jax.random.randint(own_keys[4], (NBLOCKS, SPB), 0, NSTYPE), jax.random.fold_in(own_keys[4], 1), 0, NSTYPE - 1).astype(jnp.int32),
        "trans": scatter_about(streams_of[5], (NTYPE, COEF, COEF), COEF ** -0.5, 0.25, jnp.float32),
        "coup": scatter_about(streams_of[6], (NTYPE, SPB, SPB), SPB ** -0.5, 0.5, jnp.float32),
        "tmat": scatter_about(streams_of[7], (NSTYPE, COEF, COEF), (4 * COEF) ** -0.5, 0.125, jnp.float32),
    }


def operator_apply(vector, nbr_block, nbr_type, nbr_count, sphere_type, trans, coup, tmat):

    def block_image(items):
        near_ids, pair_kinds, live_count, sphere_kinds = items
        sources = vector[near_ids]
        moved = jnp.einsum('kij,kjs->kis', trans[pair_kinds], sources, precision=lax.Precision.HIGHEST)
        coupled = jnp.einsum('kis,kts->kit', moved, coup[pair_kinds], precision=lax.Precision.HIGHEST)
        active = (jnp.arange(NBR, dtype=jnp.int32) < live_count).astype(jnp.float32)
        summed = lax.optimization_barrier(jnp.sum(active[:, None, None] * coupled, axis=0))
        scattered = jnp.einsum('tij,js->tis', tmat, summed, precision=lax.Precision.HIGHEST)
        onehot = (sphere_kinds[None, :] == jnp.arange(NSTYPE, dtype=jnp.int32)[:, None]).astype(jnp.float32)
        return lax.optimization_barrier(jnp.sum(onehot[:, None, :] * scattered, axis=0))
    images = lax.map(block_image, (nbr_block, nbr_type, nbr_count, sphere_type))
    return vector - images

def arnoldi(vectors, vector, tables):
    image = operator_apply(vector, *tables)
    total_cells = float(NBLOCKS * COEF * SPB)
    coeffs = jnp.einsum('kbcs,bcs->k', vectors, image, precision=lax.Precision.HIGHEST) / total_cells
    remainder = image - jnp.einsum('k,kbcs->bcs', coeffs, vectors, precision=lax.Precision.HIGHEST)
    norm_value = jnp.sqrt(jnp.sum(remainder * remainder) / total_cells + 1e-06)
    return (remainder / norm_value, jnp.concatenate([coeffs, norm_value[None]]))

def reference(basis, nbr_block, nbr_type, nbr_count, sphere_type, trans, coup, tmat):
    tables = (nbr_block, nbr_type, nbr_count, sphere_type, trans, coup, tmat)
    first_new, hess_first = arnoldi(basis, basis[KRY - 1], tables)
    extended = jnp.concatenate([basis, first_new[None]], axis=0)
    second_new, hess_second = arnoldi(extended, first_new, tables)
    return (jnp.stack([first_new, second_new]), hess_first, hess_second)
```

```python
import functools

import jax
import jax.numpy as jnp
import numpy as np
from jax import lax
from jax.experimental import pallas as pl
from jax.experimental.pallas import tpu as pltpu
from jax.sharding import PartitionSpec as P

GB = ("groups", "blk")
PLANE = 8
LANES = 128
F32 = jnp.float32
BF16 = jnp.bfloat16
MESH = pl.DeviceIdType.MESH


def chunk_rows(coef):
    return [(c, min(LANES, coef - c)) for c in range(0, coef, LANES)]


def lane_tables(most):
    one = most
    table = np.zeros((8, LANES), np.int32)
    table[0:2, :] = most + 1
    lane_of = {}
    for i in range(most):
        table[0:3, i] = (i, one, -2)
    table[0:3, most] = (one, one, 1)
    at = most + 1
    for i in range(most):
        for j in range(i, most):
            table[0:3, at] = (i, j, 1 if i == j else 2)
            lane_of[i, j] = at
            at += 1
    return table, lane_of, at


def halves(x):
    high = x.astype(BF16)
    return high, (x - high.astype(F32)).astype(BF16)


def kernel(
    n_blk,
    cells,
    lane_of,
    basis_hbm,
    nbr_block,
    nbr_type,
    nbr_count,
    sphere_type,
    table,
    trans_hbm,
    coup_hbm,
    tmat_hbm,
    new_hbm,
    hess_ref,
    wins,
    stack,
    tr32,
    tm32,
    cp32,
    tr3,
    tm3,
    cp2,
    mix3,
    sum3,
    acc,
    image,
    rows_ref,
    plane_buf,
    ring_buf,
    weights,
    tr_sem,
    in_sem,
    out_sem,
    halo_send,
    halo_recv,
    plane_send,
    plane_recv,
    ring_send,
    ring_recv,
):
    n_vec, n_loc, coef, sph = basis_hbm.shape
    kinds = trans_hbm.shape[0]
    s_kinds = tmat_hbm.shape[0]
    slots = nbr_block.shape[1]
    most = n_vec + 1
    chunks = chunk_rows(coef)
    n_ring = n_blk // PLANE
    window = 3 * n_loc

    me = lax.axis_index("blk")
    z = me // PLANE
    q = me % PLANE
    left, right = me - 1, me + 1
    has_left, has_right = me > 0, me < n_blk - 1
    far_left = jnp.logical_and(q == 0, has_left)
    far_right = jnp.logical_and(q == PLANE - 1, has_right)

    own = pltpu.make_async_copy(
        basis_hbm.at[n_vec - 1], wins.at[0, pl.ds(n_loc, n_loc)], in_sem.at[0]
    )
    own.start()
    cp_copy = pltpu.make_async_copy(coup_hbm, cp32, in_sem.at[1])
    cp_copy.start()
    for t in range(kinds):
        pltpu.make_async_copy(trans_hbm.at[t], tr32.at[t], tr_sem.at[t]).start()
    stack_copy = pltpu.make_async_copy(basis_hbm, stack, in_sem.at[2])
    stack_copy.start()
    tm_copy = pltpu.make_async_copy(tmat_hbm, tm32, in_sem.at[3])
    tm_copy.start()

    barrier = pltpu.get_barrier_semaphore()

    def greet(target):
        pl.semaphore_signal(barrier, inc=1, device_id={"blk": target}, device_id_type=MESH)

    def plane_peer(d):
        return z * PLANE + (q + d) % PLANE

    def ring_peer(d):
        return ((z + d) % n_ring) * PLANE + q

    for d in range(1, PLANE):
        greet(plane_peer(d))
    for d in range(1, n_ring):
        greet(ring_peer(d))

    @pl.when(far_left)
    def _():
        greet(left)

    @pl.when(far_right)
    def _():
        greet(right)

    first_block = me * n_loc
    for b in range(n_loc):
        keys = []
        for k in range(slots):
            row = nbr_block[b, k] - first_block + n_loc
            keys.append(jnp.where(k < nbr_count[b], nbr_type[b, k] * window + row, -1))
        for t in range(kinds):
            for p in range(b, b + 2 * n_loc + 1):
                hits = [jnp.where(key == t * window + p, 1, 0) for key in keys]
                while len(hits) > 1:
                    hits = [a + c for a, c in zip(hits[::2], hits[1::2])] + (
                        [hits[-1]] if len(hits) % 2 else []
                    )
                weights[(b * kinds + t) * window + p] = hits[0].astype(F32)

    pl.semaphore_wait(
        barrier,
        PLANE + n_ring - 2 + far_left.astype(jnp.int32) + far_right.astype(jnp.int32),
    )

    def halo(step, side, r):
        lo, n = chunks[r]
        to = 0 if side == 0 else 2 * n_loc
        return pltpu.make_async_remote_copy(
            src_ref=wins.at[step, pl.ds(n_loc, n_loc), pl.ds(lo, n)],
            dst_ref=wins.at[step, pl.ds(to, n_loc), pl.ds(lo, n)],
            send_sem=halo_send.at[step, side, r],
            recv_sem=halo_recv.at[step, side, r],
            device_id={"blk": right if side == 0 else left},
            device_id_type=MESH,
        )

    def halo_start(step, r):
        @pl.when(has_right)
        def _():
            halo(step, 0, r).start()

        @pl.when(has_left)
        def _():
            halo(step, 1, r).start()

    def halo_wait(step, r):
        @pl.when(has_left)
        def _():
            halo(step, 0, r).wait_recv()

        @pl.when(has_right)
        def _():
            halo(step, 1, r).wait_recv()

    own.wait()
    for r in range(len(chunks)):
        halo_start(0, r)

    @pl.when(jnp.logical_not(has_left))
    def _():
        wins[0, 0:n_loc] = jnp.zeros((n_loc, coef, sph), F32)
        wins[1, 0:n_loc] = jnp.zeros((n_loc, coef, sph), F32)

    @pl.when(jnp.logical_not(has_right))
    def _():
        wins[0, 2 * n_loc :] = jnp.zeros((n_loc, coef, sph), F32)
        wins[1, 2 * n_loc :] = jnp.zeros((n_loc, coef, sph), F32)

    rows_ref[...] = jnp.zeros_like(rows_ref)
    sum3[...] = jnp.zeros_like(sum3)

    cp_copy.wait()

    def split_coup(t, carry):
        high, low = halves(cp32[t].T)
        cp2[t, 0:sph, 0:sph] = high
        cp2[t, 0:sph, sph:] = low
        cp2[t, sph:, 0:sph] = high
        cp2[t, sph:, sph:] = jnp.zeros_like(low)
        return carry

    lax.fori_loop(0, kinds, split_coup, 0)

    def split_left(x, n):
        if n < LANES:
            x = jnp.concatenate([x, jnp.zeros((coef, LANES - n), F32)], axis=1)
        return halves(x)

    def split_trans(t, carry):
        pltpu.make_async_copy(trans_hbm.at[t], tr32.at[t], tr_sem.at[t]).wait()
        for r, (lo, n) in enumerate(chunks):
            high, low = split_left(tr32[t, :, lo : lo + n], n)
            for i, part in enumerate((high, low, high)):
                at = pl.multiple_of((t * 3 + i) * LANES, LANES)
                tr3[r, :, pl.ds(at, LANES)] = part
        return carry

    lax.fori_loop(0, kinds, split_trans, 0)

    stack_copy.wait()
    pairs = [(i, j) for i in range(n_vec) for j in range(i, n_vec)]

    def gram_step(g, sums):
        at = pl.multiple_of(g * 8, 8)
        sums = list(sums)
        for b in range(n_loc):
            vs = [stack[i, b, pl.ds(at, 8), :] for i in range(n_vec)]
            for c, (i, j) in enumerate(pairs):
                sums[c] = sums[c] + vs[i] * vs[j]
        return tuple(sums)

    gram = lax.fori_loop(
        0, coef // 8, gram_step, tuple(jnp.zeros((8, sph), F32) for _ in pairs)
    )
    for c, (i, j) in enumerate(pairs):
        at = lane_of[i, j]
        rows_ref[at : at + 1, :] = jnp.sum(gram[c], axis=0, keepdims=True)

    tm_copy.wait()

    def split_tmat(t, carry):
        for r, (lo, n) in enumerate(chunks):
            high, low = split_left(tm32[t, :, lo : lo + n], n)
            for i, part in enumerate((high, low, high)):
                at = (r * 3 + i) * LANES
                tm3[t, :, at : at + LANES] = part
        return carry

    lax.fori_loop(0, s_kinds, split_tmat, 0)

    def mix(step, r):
        lo, n = chunks[r]
        for t in range(kinds):
            blocks = []
            for b in range(n_loc):
                total = None
                for p in range(b, b + 2 * n_loc + 1):
                    term = weights[(b * kinds + t) * window + p] * wins[step, p, lo : lo + n, :]
                    total = term if total is None else total + term
                blocks.append(total)
            high, low = halves(jnp.concatenate(blocks, axis=0))
            both = jnp.dot(
                jnp.concatenate([high, low], axis=1), cp2[t], preferred_element_type=F32
            )
            high, low = halves(both[:, :sph] + both[:, sph:])
            for i, part in enumerate((high, high, low)):
                at = (t * 3 + i) * LANES
                for b in range(n_loc):
                    mix3[r % 2, at : at + n, b * sph : (b + 1) * sph] = part[b * n : (b + 1) * n]

    def apply(step):
        halo_wait(step, 0)
        mix(step, 0)
        for r in range(len(chunks)):
            if r + 1 < len(chunks):
                halo_wait(step, r + 1)
                mix(step, r + 1)
            part = jnp.dot(tr3[r], mix3[r % 2], preferred_element_type=F32)
            if r == 0:
                acc[...] = part
            else:
                acc[...] += part
        for r, (lo, n) in enumerate(chunks):
            high, low = halves(acc[lo : lo + n, :])
            for i, part in enumerate((high, high, low)):
                at = (r * 3 + i) * LANES
                sum3[at : at + n, :] = part
        types = jnp.concatenate([sphere_type[b : b + 1, :] for b in range(n_loc)], axis=1)
        for t in range(s_kinds):
            part = jnp.dot(tm3[t], sum3[...], preferred_element_type=F32)
            here = jnp.broadcast_to(types == t, part.shape)
            if t == 0:
                acc[...] = jnp.where(here, part, 0.0)
            else:
                acc[...] = jnp.where(here, part, acc[...])
        for b in range(n_loc):
            image[b] = wins[step, n_loc + b] - acc[:, b * sph : (b + 1) * sph]

    GROUP = 40 if coef % 40 == 0 else 8

    def vector_rows(i, b, at):
        if i < n_vec:
            return stack[i, b, pl.ds(at, GROUP), :]
        return wins[1, n_loc + b, pl.ds(at, GROUP), :]

    def fold(x):
        return jnp.sum(x.reshape(GROUP // 8, 8, sph), axis=0)

    def dots(lefts, right_rows, extra):
        def body(g, sums):
            at = pl.multiple_of(g * GROUP, 8)
            sums = list(sums)
            for b in range(n_loc):
                w = right_rows(b, at)
                for c, i in enumerate(lefts):
                    sums[c] = sums[c] + fold(vector_rows(i, b, at) * w)
                if extra:
                    sums[-1] = sums[-1] + fold(w * w)
            return tuple(sums)

        zero = jnp.zeros((8, sph), F32)
        return lax.fori_loop(
            0, coef // GROUP, body, tuple(zero for _ in range(len(lefts) + int(extra)))
        )

    def lanes_of_rows():
        x = rows_ref[...]
        col = jnp.sum(x, axis=1, keepdims=True)
        row_id = lax.broadcasted_iota(jnp.int32, x.shape, 0)
        lane_id = lax.broadcasted_iota(jnp.int32, x.shape, 1)
        return jnp.sum(jnp.where(row_id == lane_id, col, 0.0), axis=0, keepdims=True)

    def plane_copy(step, d):
        return pltpu.make_async_remote_copy(
            src_ref=plane_buf.at[step, q],
            dst_ref=plane_buf.at[step, q],
            send_sem=plane_send.at[step, d],
            recv_sem=plane_recv.at[step, d],
            device_id={"blk": plane_peer(d)},
            device_id_type=MESH,
        )

    def ring_copy(step, d):
        return pltpu.make_async_remote_copy(
            src_ref=ring_buf.at[step, z],
            dst_ref=ring_buf.at[step, z],
            send_sem=ring_send.at[step, d],
            recv_sem=ring_recv.at[step, d],
            device_id={"blk": ring_peer(d)},
            device_id_type=MESH,
        )

    def all_reduce(step, x):
        plane_buf[step, q] = x
        for d in range(1, PLANE):
            plane_copy(step, d).start()
        for d in range(1, PLANE):
            plane_copy(step, d).wait_recv()
        ring_buf[step, z] = functools.reduce(
            jnp.add, [plane_buf[step, i] for i in range(PLANE)]
        )
        order = sorted(range(1, n_ring), key=lambda d: -min(d, n_ring - d))
        for d in order:
            ring_copy(step, d).start()
        for d in order:
            ring_copy(step, d).wait_recv()
        return functools.reduce(jnp.add, [ring_buf[step, i] for i in range(n_ring)])

    def orthogonal(step, n_used, store):
        sums = dots(range(n_used), lambda b, at: image[b, pl.ds(at, GROUP), :], True)
        for i in range(n_used):
            rows_ref[i : i + 1, :] = jnp.sum(sums[i], axis=0, keepdims=True)
        rows_ref[most : most + 1, :] = jnp.sum(sums[n_used], axis=0, keepdims=True)
        total = all_reduce(step, lanes_of_rows())
        coeffs = total * (1.0 / cells)
        spread = [jnp.broadcast_to(coeffs[:, i : i + 1], (1, LANES)) for i in range(n_used)]

        def factor(which):
            out = jnp.where(which == most, 1.0, 0.0)
            for i in range(n_used):
                out = jnp.where(which == i, spread[i], out)
            return out

        share = total * table[2:3, :].astype(F32)
        share = share * factor(table[0:1, :]) * factor(table[1:2, :])
        squares = jnp.sum(share, axis=1, keepdims=True)
        norm = jnp.sqrt(jnp.maximum(squares, 0.0) * (1.0 / cells) + 1e-6)
        lane = lax.broadcasted_iota(jnp.int32, (1, LANES), 1)
        norm_row = jnp.broadcast_to(norm, (1, LANES))
        hess_ref[step : step + 1, :] = jnp.where(lane == n_used, norm_row, coeffs)
        inverse = jnp.broadcast_to(1.0 / norm_row, (8, LANES))
        wide = [jnp.broadcast_to(s, (8, LANES)) for s in spread]

        def rows(lo, n):
            def body(g, carry):
                at = pl.multiple_of(lo + g * 8, 8)
                for b in range(n_loc):
                    u = image[b, pl.ds(at, 8), :]
                    for i in range(n_used):
                        if i < n_vec:
                            u = u - wide[i] * stack[i, b, pl.ds(at, 8), :]
                        else:
                            u = u - wide[i] * wins[1, n_loc + b, pl.ds(at, 8), :]
                    store(b, at, u * inverse)
                return carry

            lax.fori_loop(0, n // 8, body, 0, unroll=4)

        return rows

    apply(0)

    def store_first(b, at, value):
        wins[1, n_loc + b, pl.ds(at, 8), :] = value

    rows = orthogonal(0, n_vec, store_first)
    for r, (lo, n) in enumerate(chunks):
        rows(lo, n)
        halo_start(1, r)
    out_first = pltpu.make_async_copy(
        wins.at[1, pl.ds(n_loc, n_loc)], new_hbm.at[0], out_sem.at[0]
    )
    out_first.start()

    def first_rows(b, at):
        return wins[1, n_loc + b, pl.ds(at, GROUP), :]

    new_pairs = dots(range(n_vec), first_rows, True)
    for i in range(most):
        at = lane_of[i, n_vec]
        rows_ref[at : at + 1, :] = jnp.sum(new_pairs[i], axis=0, keepdims=True)

    apply(1)

    def store_second(b, at, value):
        image[b, pl.ds(at, 8), :] = value

    rows = orthogonal(1, most, store_second)
    rows(0, coef)
    out_second = pltpu.make_async_copy(image, new_hbm.at[1], out_sem.at[1])
    out_second.start()

    for step in range(2):
        for r in range(len(chunks)):

            @pl.when(has_right)
            def _():
                halo(step, 0, r).wait_send()

            @pl.when(has_left)
            def _():
                halo(step, 1, r).wait_send()

        for d in range(1, PLANE):
            plane_copy(step, d).wait_send()
        for d in range(1, n_ring):
            ring_copy(step, d).wait_send()
    out_first.wait()
    out_second.wait()


def shards(n_blk, basis, nbr_block, nbr_type, nbr_count, sphere_type, trans, coup, tmat):
    n_vec, n_loc, coef, sph = basis.shape
    kinds, s_kinds = trans.shape[0], tmat.shape[0]
    chunks = chunk_rows(coef)
    n_ring = n_blk // PLANE
    table, lane_of, used = lane_tables(n_vec + 1)
    cells = float(n_blk * n_loc * coef * sph)
    any_space = pl.BlockSpec(memory_space=pl.ANY)
    smem = pl.BlockSpec(memory_space=pltpu.SMEM)
    vmem = pl.BlockSpec(memory_space=pltpu.VMEM)
    dma = pltpu.SemaphoreType.DMA
    wide = n_loc * sph
    new, hess = pl.pallas_call(
        functools.partial(kernel, n_blk, cells, lane_of),
        out_shape=(
            jax.ShapeDtypeStruct((2, n_loc, coef, sph), F32),
            jax.ShapeDtypeStruct((8, LANES), F32),
        ),
        in_specs=[any_space, smem, smem, smem, vmem, vmem, any_space, any_space, any_space],
        out_specs=(any_space, vmem),
        scratch_shapes=[
            pltpu.VMEM((2, 3 * n_loc, coef, sph), F32),
            pltpu.VMEM((n_vec, n_loc, coef, sph), F32),
            pltpu.VMEM(trans.shape, F32),
            pltpu.VMEM(tmat.shape, F32),
            pltpu.VMEM(coup.shape, F32),
            pltpu.VMEM((len(chunks), coef, kinds * 3 * LANES), BF16),
            pltpu.VMEM((s_kinds, coef, len(chunks) * 3 * LANES), BF16),
            pltpu.VMEM((kinds, 2 * sph, 2 * sph), BF16),
            pltpu.VMEM((2, kinds * 3 * LANES, wide), BF16),
            pltpu.VMEM((len(chunks) * 3 * LANES, wide), BF16),
            pltpu.VMEM((coef, wide), F32),
            pltpu.VMEM((n_loc, coef, sph), F32),
            pltpu.VMEM(((used + 7) // 8 * 8, LANES), F32),
            pltpu.VMEM((2, PLANE, 1, LANES), F32),
            pltpu.VMEM((2, n_ring, 1, LANES), F32),
            pltpu.SMEM((n_loc * kinds * 3 * n_loc,), F32),
            dma((kinds,)),
            dma((4,)),
            dma((2,)),
            dma((2, 2, len(chunks))),
            dma((2, 2, len(chunks))),
            dma((2, PLANE)),
            dma((2, PLANE)),
            dma((2, n_ring)),
            dma((2, n_ring)),
        ],
        compiler_params=pltpu.CompilerParams(
            collective_id=0, has_side_effects=True, vmem_limit_bytes=60 * 1024 * 1024
        ),
    )(
        basis,
        nbr_block,
        nbr_type,
        nbr_count,
        sphere_type,
        jnp.asarray(table),
        trans,
        coup,
        tmat,
    )
    return new, hess[0, : n_vec + 1], hess[1, : n_vec + 2]


def solution(mesh):
    return jax.shard_map(
        functools.partial(shards, mesh.shape["blk"]),
        mesh=mesh,
        in_specs=(
            P(None, GB, None, None),
            P(GB, None),
            P(GB, None),
            P(GB),
            P(GB, None),
            P(),
            P(),
            P(),
        ),
        out_specs=(P(None, GB, None, None), P("groups"), P("groups")),
        check_vma=False,
    )
```

```python
import functools

import jax
import jax.numpy as jnp
import numpy as np
from jax import lax
from jax.experimental import pallas as pl
from jax.experimental.pallas import tpu as pltpu
from jax.sharding import PartitionSpec as P

GB = ("groups", "blk")
PLANE = 8
LANES = 128
F32 = jnp.float32
BF16 = jnp.bfloat16
MESH = pl.DeviceIdType.MESH


def chunk_rows(coef):
    return [(c, min(LANES, coef - c)) for c in range(0, coef, LANES)]


def lane_tables(most):
    one = most
    table = np.zeros((8, LANES), np.int32)
    table[0:2, :] = most + 1
    lane_of = {}
    for i in range(most):
        table[0:3, i] = (i, one, -2)
    table[0:3, most] = (one, one, 1)
    at = most + 1
    for i in range(most):
        for j in range(i, most):
            table[0:3, at] = (i, j, 1 if i == j else 2)
            lane_of[i, j] = at
            at += 1
    return table, lane_of, at


def halves(x):
    high = x.astype(BF16)
    return high, (x - high.astype(F32)).astype(BF16)


def kernel(
    n_blk,
    cells,
    lane_of,
    basis_hbm,
    nbr_block_hbm,
    nbr_type_hbm,
    nbr_count_hbm,
    sphere_type_hbm,
    table_hbm,
    trans_hbm,
    coup_hbm,
    tmat_hbm,
    new_ref,
    hess_ref,
    nbr_block,
    nbr_type,
    nbr_count,
    sphere_type,
    table,
    weights,
    wins,
    stack,
    tr32,
    tm32,
    cp32,
    tr3,
    tm3,
    cp2,
    mix3,
    sum3,
    acc,
    image,
    rows_ref,
    plane_buf,
    ring_buf,
    tr_sem,
    in_sem,
    halo_send,
    halo_recv,
    plane_send,
    plane_recv,
    ring_send,
    ring_recv,
):
    n_vec, n_loc, coef, sph = basis_hbm.shape
    kinds = trans_hbm.shape[0]
    s_kinds = tmat_hbm.shape[0]
    slots = nbr_block_hbm.shape[1]
    most = n_vec + 1
    chunks = chunk_rows(coef)
    n_ring = n_blk // PLANE
    window = 3 * n_loc

    me = lax.axis_index("blk")
    z = me // PLANE
    q = me % PLANE
    left, right = me - 1, me + 1
    has_left, has_right = me > 0, me < n_blk - 1
    far_left = jnp.logical_and(q == 0, has_left)
    far_right = jnp.logical_and(q == PLANE - 1, has_right)

    own = pltpu.make_async_copy(
        basis_hbm.at[n_vec - 1], wins.at[0, pl.ds(n_loc, n_loc)], in_sem.at[0]
    )
    own.start()
    small = [
        pltpu.make_async_copy(src, dst, in_sem.at[4 + i])
        for i, (src, dst) in enumerate(
            (
                (nbr_block_hbm, nbr_block),
                (nbr_type_hbm, nbr_type),
                (nbr_count_hbm, nbr_count),
                (sphere_type_hbm, sphere_type),
                (table_hbm, table),
            )
        )
    ]
    for copy in small:
        copy.start()
    cp_copy = pltpu.make_async_copy(coup_hbm, cp32, in_sem.at[1])
    cp_copy.start()

    def trans_copy(r):
        lo, n = chunks[r]
        return pltpu.make_async_copy(
            trans_hbm.at[:, :, pl.ds(lo, n)], tr32.at[:, :, pl.ds(lo, n)], tr_sem.at[r]
        )

    for r in range(len(chunks)):
        trans_copy(r).start()
    stack_copy = pltpu.make_async_copy(basis_hbm, stack, in_sem.at[2])
    stack_copy.start()
    tm_copy = pltpu.make_async_copy(tmat_hbm, tm32, in_sem.at[3])
    tm_copy.start()

    barrier = pltpu.get_barrier_semaphore()

    def greet(target):
        pl.semaphore_signal(barrier, inc=1, device_id={"blk": target}, device_id_type=MESH)

    def plane_peer(d):
        return z * PLANE + (q + d) % PLANE

    def ring_peer(d):
        return ((z + d) % n_ring) * PLANE + q

    for d in range(1, PLANE):
        greet(plane_peer(d))
    for d in range(1, n_ring):
        greet(ring_peer(d))

    @pl.when(far_left)
    def _():
        greet(left)

    @pl.when(far_right)
    def _():
        greet(right)

    pl.semaphore_wait(
        barrier,
        PLANE + n_ring - 2 + far_left.astype(jnp.int32) + far_right.astype(jnp.int32),
    )

    def halo(step, side, r):
        lo, n = chunks[r]
        to = 0 if side == 0 else 2 * n_loc
        return pltpu.make_async_remote_copy(
            src_ref=wins.at[step, pl.ds(n_loc, n_loc), pl.ds(lo, n)],
            dst_ref=wins.at[step, pl.ds(to, n_loc), pl.ds(lo, n)],
            send_sem=halo_send.at[step, side, r],
            recv_sem=halo_recv.at[step, side, r],
            device_id={"blk": right if side == 0 else left},
            device_id_type=MESH,
        )

    def halo_start(step, r):
        @pl.when(has_right)
        def _():
            halo(step, 0, r).start()

        @pl.when(has_left)
        def _():
            halo(step, 1, r).start()

    def halo_wait(step, r):
        @pl.when(has_left)
        def _():
            halo(step, 0, r).wait_recv()

        @pl.when(has_right)
        def _():
            halo(step, 1, r).wait_recv()

    own.wait()
    for r in range(len(chunks)):
        halo_start(0, r)

    @pl.when(jnp.logical_not(has_left))
    def _():
        wins[0, 0:n_loc] = jnp.zeros((n_loc, coef, sph), F32)
        wins[1, 0:n_loc] = jnp.zeros((n_loc, coef, sph), F32)

    @pl.when(jnp.logical_not(has_right))
    def _():
        wins[0, 2 * n_loc :] = jnp.zeros((n_loc, coef, sph), F32)
        wins[1, 2 * n_loc :] = jnp.zeros((n_loc, coef, sph), F32)

    for copy in small:
        copy.wait()
    first_block = me * n_loc
    slot_id = lax.broadcasted_iota(jnp.int32, (1, slots), 1)
    use_id = lax.broadcasted_iota(jnp.int32, (kinds * window, slots), 0)
    for b in range(n_loc):
        use = nbr_type[b : b + 1, :] * window + (nbr_block[b : b + 1, :] - first_block + n_loc)
        use = jnp.where(slot_id < nbr_count[b], use, -1)
        hits = jnp.sum(jnp.where(use_id == use, 1.0, 0.0), axis=1, keepdims=True)
        weights[b] = jnp.broadcast_to(hits, (kinds * window, LANES))

    rows_ref[...] = jnp.zeros_like(rows_ref)
    sum3[...] = jnp.zeros_like(sum3)

    cp_copy.wait()

    def split_coup(t, carry):
        high, low = halves(cp32[t].T)
        cp2[t, 0, 0:sph] = high
        cp2[t, 0, sph:] = high
        cp2[t, 1, 0:sph] = low
        cp2[t, 1, sph:] = jnp.zeros_like(low)
        return carry

    lax.fori_loop(0, kinds, split_coup, 0, unroll=4)

    def split_left(x, n):
        if n < LANES:
            x = jnp.concatenate([x, jnp.zeros((coef, LANES - n), F32)], axis=1)
        return halves(x)

    def split_trans(r):
        lo, n = chunks[r]
        for t in range(kinds):
            high, low = split_left(tr32[t, :, lo : lo + n], n)
            tr3[r, 0, t] = high
            tr3[r, 1, t] = low

    def split_tmat():
        for t in range(s_kinds):
            for r, (lo, n) in enumerate(chunks):
                high, low = split_left(tm32[t, :, lo : lo + n], n)
                tm3[t, 0, r] = high
                tm3[t, 1, r] = low

    depth = len(chunks) * LANES
    pairs = [(i, j) for i in range(n_vec) for j in range(i, n_vec)]

    def gram_step(g, sums):
        at = pl.multiple_of(g * 8, 8)
        sums = list(sums)
        for b in range(n_loc):
            vs = [stack[i, b, pl.ds(at, 8), :] for i in range(n_vec)]
            for c, (i, j) in enumerate(pairs):
                sums[c] = sums[c] + vs[i] * vs[j]
        return tuple(sums)

    def basis_pairs():
        gram = lax.fori_loop(
            0, coef // 8, gram_step, tuple(jnp.zeros((8, sph), F32) for _ in pairs)
        )
        for c, (i, j) in enumerate(pairs):
            at = lane_of[i, j]
            rows_ref[at : at + 1, :] = jnp.sum(gram[c], axis=0, keepdims=True)

    def three(left, right):
        high, low = right
        part = jnp.dot(left[0], high, preferred_element_type=F32)
        part += jnp.dot(left[1], high, preferred_element_type=F32)
        part += jnp.dot(left[0], low, preferred_element_type=F32)
        return part

    def wide_left(ref, lead, count, rows):
        return [
            jnp.concatenate([ref[(*lead, i, k, rows)] for k in range(count)], axis=1)
            for i in range(2)
        ]

    def wide_right(ref, lead):
        return [
            jnp.concatenate([ref[(*lead, i, b)] for b in range(n_loc)], axis=1)
            for i in range(2)
        ]

    half = coef // 2

    def product(r):
        for lo in (0, half):
            left = wide_left(tr3, (r,), kinds, slice(lo, lo + half))
            part = three(left, wide_right(mix3, (r % 2,)))
            if r == 0:
                acc[lo : lo + half] = part
            else:
                acc[lo : lo + half] += part

    def mix(step, r):
        lo, n = chunks[r]
        for t in range(kinds):
            blocks = []
            for b in range(n_loc):
                total = None
                for p in range(b, b + 2 * n_loc + 1):
                    c = t * window + p
                    term = weights[b, c : c + 1, :] * wins[step, p, lo : lo + n, :]
                    total = term if total is None else total + term
                blocks.append(total)
            high, low = halves(jnp.concatenate(blocks, axis=0))
            both = jnp.dot(
                jnp.concatenate([high, low], axis=1),
                jnp.concatenate([cp2[t, 0], cp2[t, 1]], axis=1),
                preferred_element_type=F32,
            )
            high, low = halves(both[:, :sph] + both[:, sph:])
            for i, part in enumerate((high, low)):
                for b in range(n_loc):
                    mix3[r % 2, i, b, t * LANES : t * LANES + n] = part[b * n : (b + 1) * n]

    def apply(step):
        last = len(chunks) - 1
        for r in range(len(chunks)):
            if step == 0:
                trans_copy(r).wait()
            halo_wait(step, r)
            if step == 0:
                split_trans(r)
            mix(step, r)
            if r > 0:
                product(r - 1)
        if step == 0:
            tm_copy.wait()
            stack_copy.wait()

        @pl.when(me >= 0)
        def _():
            product(last)
            if step == 0:
                split_tmat()

        for lo, n in chunks:
            high, low = halves(acc[lo : lo + n, :])
            for b in range(n_loc):
                sum3[0, b, lo : lo + n] = high[:, b * sph : (b + 1) * sph]
                sum3[1, b, lo : lo + n] = low[:, b * sph : (b + 1) * sph]
        types = jnp.concatenate([sphere_type[b : b + 1, :] for b in range(n_loc)], axis=1)

        def scatter(i, carry):
            for t in (2 * i, 2 * i + 1):
                part = three(
                    wide_left(tm3, (t,), len(chunks), slice(None)), wide_right(sum3, ())
                )
                here = jnp.broadcast_to(types == t, part.shape)
                acc[...] = jnp.where(here, part, acc[...])
            return carry

        lax.fori_loop(0, s_kinds // 2, scatter, 0)
        for b in range(n_loc):
            image[b] = wins[step, n_loc + b] - acc[:, b * sph : (b + 1) * sph]

    GROUP = 40 if coef % 40 == 0 else 8

    def vector_rows(i, b, at):
        if i < n_vec:
            return stack[i, b, pl.ds(at, GROUP), :]
        return wins[1, n_loc + b, pl.ds(at, GROUP), :]

    def fold(x):
        return jnp.sum(x.reshape(GROUP // 8, 8, sph), axis=0)

    def dots(lefts, right_rows, extra):
        def body(g, sums):
            at = pl.multiple_of(g * GROUP, 8)
            sums = list(sums)
            for b in range(n_loc):
                w = right_rows(b, at)
                for c, i in enumerate(lefts):
                    sums[c] = sums[c] + fold(vector_rows(i, b, at) * w)
                if extra:
                    sums[-1] = sums[-1] + fold(w * w)
            return tuple(sums)

        zero = jnp.zeros((8, sph), F32)
        return lax.fori_loop(
            0, coef // GROUP, body, tuple(zero for _ in range(len(lefts) + int(extra)))
        )

    def lanes_of_rows():
        x = rows_ref[...]
        col = jnp.sum(x, axis=1, keepdims=True)
        row_id = lax.broadcasted_iota(jnp.int32, x.shape, 0)
        lane_id = lax.broadcasted_iota(jnp.int32, x.shape, 1)
        return jnp.sum(jnp.where(row_id == lane_id, col, 0.0), axis=0, keepdims=True)

    def plane_copy(step, d):
        return pltpu.make_async_remote_copy(
            src_ref=plane_buf.at[step, q],
            dst_ref=plane_buf.at[step, q],
            send_sem=plane_send.at[step, d],
            recv_sem=plane_recv.at[step, d],
            device_id={"blk": plane_peer(d)},
            device_id_type=MESH,
        )

    def ring_copy(step, d):
        return pltpu.make_async_remote_copy(
            src_ref=ring_buf.at[step, z],
            dst_ref=ring_buf.at[step, z],
            send_sem=ring_send.at[step, d],
            recv_sem=ring_recv.at[step, d],
            device_id={"blk": ring_peer(d)},
            device_id_type=MESH,
        )

    def all_reduce(step, x, meanwhile):
        plane_buf[step, q] = x
        for d in range(1, PLANE):
            plane_copy(step, d).start()
        for d in range(1, PLANE):
            plane_copy(step, d).wait_recv()
        ring_buf[step, z] = functools.reduce(
            jnp.add, [plane_buf[step, i] for i in range(PLANE)]
        )
        order = sorted(range(1, n_ring), key=lambda d: -min(d, n_ring - d))
        for d in order:
            ring_copy(step, d).start()
        meanwhile()
        for d in order:
            ring_copy(step, d).wait_recv()
        return functools.reduce(jnp.add, [ring_buf[step, i] for i in range(n_ring)])

    def reduced(step, n_used, meanwhile):
        sums = dots(range(n_used), lambda b, at: image[b, pl.ds(at, GROUP), :], True)
        for i in range(n_used):
            rows_ref[i : i + 1, :] = jnp.sum(sums[i], axis=0, keepdims=True)
        rows_ref[most : most + 1, :] = jnp.sum(sums[n_used], axis=0, keepdims=True)
        return all_reduce(step, lanes_of_rows(), meanwhile) * (1.0 / cells)

    def spread(row, i):
        return jnp.broadcast_to(row[:, i : i + 1], (1, LANES))

    def tall(row):
        return jnp.broadcast_to(row, (8, LANES))

    def vector8(i, b, at):
        if i < n_vec:
            return stack[i, b, pl.ds(at, 8), :]
        return wins[1, n_loc + b, pl.ds(at, 8), :]

    def combine(shares, scale, store, lo, n):
        def body(g, carry):
            at = pl.multiple_of(lo + g * 8, 8)
            for b in range(n_loc):
                u = image[b, pl.ds(at, 8), :]
                for i, share in enumerate(shares):
                    u = u - share * vector8(i, b, at)
                store(b, at, u * scale)
            return carry

        lax.fori_loop(0, n // 8, body, 0, unroll=4)

    lane = lax.broadcasted_iota(jnp.int32, (1, LANES), 1)

    apply(0)
    means = reduced(0, n_vec, basis_pairs)
    first_row = means
    size2 = spread(means, most) + 1e-6
    size = jnp.sqrt(size2)
    shares = [tall(spread(means, i)) for i in range(n_vec)]
    scale = tall(1.0 / size)

    def store_first(b, at, value):
        wins[1, n_loc + b, pl.ds(at, 8), :] = value

    for r, (lo, n) in enumerate(chunks):
        combine(shares, scale, store_first, lo, n)
        halo_start(1, r)

    def first_rows(b, at):
        return wins[1, n_loc + b, pl.ds(at, GROUP), :]

    new_pairs = dots(range(n_vec), first_rows, True)
    for i in range(most):
        at = lane_of[i, n_vec]
        rows_ref[at : at + 1, :] = jnp.sum(new_pairs[i], axis=0, keepdims=True)

    apply(1)
    means = reduced(1, most, lambda: None)
    norm1 = jnp.sqrt(size2 * spread(means, lane_of[n_vec, n_vec]) + 1e-6)
    ratio = size / norm1
    parts = [spread(means, i) for i in range(n_vec)]
    parts.append(ratio * ratio * spread(means, n_vec))

    def factor(which):
        out = jnp.where(which == most, 1.0, 0.0)
        for i in range(most):
            out = jnp.where(which == i, parts[i], out)
        return out

    share = means * table[2:3, :].astype(F32)
    share = share * factor(table[0:1, :]) * factor(table[1:2, :])
    squares = jnp.broadcast_to(jnp.sum(share, axis=1, keepdims=True), (1, LANES))
    norm2 = jnp.sqrt(ratio * ratio * jnp.maximum(squares, 0.0) + 1e-6)
    hess_ref[0:1, :] = jnp.where(lane == n_vec, norm1, first_row)
    second_row = ratio * jnp.where(lane == n_vec, ratio * means, means)
    hess_ref[1:2, :] = jnp.where(lane == most, norm2, second_row)

    grow = tall(ratio)

    def store_second(b, at, value):
        new_ref[1, b, pl.ds(at, 8), :] = value
        new_ref[0, b, pl.ds(at, 8), :] = vector8(n_vec, b, at) * grow

    combine([tall(p) for p in parts], tall(ratio / norm2), store_second, 0, coef)

    for step in range(2):
        for r in range(len(chunks)):

            @pl.when(has_right)
            def _():
                halo(step, 0, r).wait_send()

            @pl.when(has_left)
            def _():
                halo(step, 1, r).wait_send()

        for d in range(1, PLANE):
            plane_copy(step, d).wait_send()
        for d in range(1, n_ring):
            ring_copy(step, d).wait_send()


def finish(new_in, hess, new_out, first, second, sem):
    store = pltpu.make_async_copy(new_in, new_out, sem)
    store.start()
    first[...] = hess[0, : first.shape[0]]
    second[...] = hess[1, : second.shape[0]]
    store.wait()


def shards(n_blk, basis, nbr_block, nbr_type, nbr_count, sphere_type, trans, coup, tmat):
    n_vec, n_loc, coef, sph = basis.shape
    kinds, s_kinds = trans.shape[0], tmat.shape[0]
    chunks = chunk_rows(coef)
    n_ring = n_blk // PLANE
    table, lane_of, used = lane_tables(n_vec + 1)
    cells = float(n_blk * n_loc * coef * sph)
    hbm = pl.BlockSpec(memory_space=pltpu.HBM)
    vmem = pl.BlockSpec(memory_space=pltpu.VMEM)
    dma = pltpu.SemaphoreType.DMA
    wide = n_loc * sph
    in_hbm = functools.partial(pltpu.with_memory_space_constraint, memory_space=pltpu.HBM)
    new, hess = pl.pallas_call(
        functools.partial(kernel, n_blk, cells, lane_of),
        out_shape=(
            jax.ShapeDtypeStruct((2, n_loc, coef, sph), F32),
            jax.ShapeDtypeStruct((8, LANES), F32),
        ),
        in_specs=[hbm] * 9,
        out_specs=(vmem, vmem),
        scratch_shapes=[
            pltpu.VMEM(nbr_block.shape, jnp.int32),
            pltpu.VMEM(nbr_type.shape, jnp.int32),
            pltpu.SMEM(nbr_count.shape, jnp.int32),
            pltpu.VMEM(sphere_type.shape, jnp.int32),
            pltpu.VMEM(table.shape, jnp.int32),
            pltpu.VMEM((n_loc, kinds * 3 * n_loc, LANES), F32),
            pltpu.VMEM((2, 3 * n_loc, coef, sph), F32),
            pltpu.VMEM((n_vec, n_loc, coef, sph), F32),
            pltpu.VMEM(trans.shape, F32),
            pltpu.VMEM(tmat.shape, F32),
            pltpu.VMEM(coup.shape, F32),
            pltpu.VMEM((len(chunks), 2, kinds, coef, LANES), BF16),
            pltpu.VMEM((s_kinds, 2, len(chunks), coef, LANES), BF16),
            pltpu.VMEM((kinds, 2, 2 * sph, sph), BF16),
            pltpu.VMEM((2, 2, n_loc, kinds * LANES, sph), BF16),
            pltpu.VMEM((2, n_loc, len(chunks) * LANES, sph), BF16),
            pltpu.VMEM((coef, wide), F32),
            pltpu.VMEM((n_loc, coef, sph), F32),
            pltpu.VMEM(((used + 7) // 8 * 8, LANES), F32),
            pltpu.VMEM((2, PLANE, 1, LANES), F32),
            pltpu.VMEM((2, n_ring, 1, LANES), F32),
            dma((len(chunks),)),
            dma((9,)),
            dma((2, 2, len(chunks))),
            dma((2, 2, len(chunks))),
            dma((2, PLANE)),
            dma((2, PLANE)),
            dma((2, n_ring)),
            dma((2, n_ring)),
        ],
        compiler_params=pltpu.CompilerParams(
            collective_id=0, has_side_effects=True, vmem_limit_bytes=52 * 1024 * 1024
        ),
    )(
        *map(
            in_hbm,
            (
                basis,
                nbr_block,
                nbr_type,
                nbr_count,
                sphere_type,
                jnp.asarray(table),
                trans,
                coup,
                tmat,
            ),
        )
    )
    return pl.pallas_call(
        finish,
        out_shape=(
            jax.ShapeDtypeStruct(new.shape, F32),
            jax.ShapeDtypeStruct((n_vec + 1,), F32),
            jax.ShapeDtypeStruct((n_vec + 2,), F32),
        ),
        in_specs=[vmem, vmem],
        out_specs=(hbm, vmem, vmem),
        scratch_shapes=[dma],
        compiler_params=pltpu.CompilerParams(vmem_limit_bytes=4 * 1024 * 1024),
    )(new, hess)


def solution(mesh):
    return jax.shard_map(
        functools.partial(shards, mesh.shape["blk"]),
        mesh=mesh,
        in_specs=(
            P(None, GB, None, None),
            P(GB, None),
            P(GB, None),
            P(GB),
            P(GB, None),
            P(),
            P(),
            P(),
        ),
        out_specs=(P(None, GB, None, None), P("groups"), P("groups")),
        check_vma=False,
    )
```

```python
import functools

import jax
import jax.numpy as jnp
import numpy as np
from jax import lax
from jax.experimental import pallas as pl
from jax.experimental.pallas import tpu as pltpu
from jax.sharding import PartitionSpec as P

GB = ("groups", "blk")
PLANE = 8
LANES = 128
F32 = jnp.float32
BF16 = jnp.bfloat16
MESH = pl.DeviceIdType.MESH


def chunk_rows(coef):
    parts = [(c, min(LANES, coef - c)) for c in range(0, coef, LANES)]
    return parts[-1:] + parts[:-1]


def lane_tables(most):
    one = most
    table = np.zeros((8, LANES), np.int32)
    table[0:2, :] = most + 1
    lane_of = {}
    for i in range(most):
        table[0:3, i] = (i, one, -2)
    table[0:3, most] = (one, one, 1)
    at = most + 1
    for i in range(most):
        for j in range(i, most):
            table[0:3, at] = (i, j, 1 if i == j else 2)
            lane_of[i, j] = at
            at += 1
    return table, lane_of, at


def halves(x):
    high = x.astype(BF16)
    return high, (x - high.astype(F32)).astype(BF16)


def kernel(
    n_blk,
    cells,
    lane_of,
    basis_hbm,
    nbr_block_hbm,
    nbr_type_hbm,
    nbr_count_hbm,
    sphere_type_hbm,
    table_hbm,
    trans_hbm,
    coup_hbm,
    tmat_hbm,
    new_ref,
    hess_ref,
    nbr_block,
    nbr_type,
    nbr_count,
    sphere_type,
    table,
    weights,
    wins,
    stack,
    tr32,
    tm32,
    cp32,
    tr3,
    tm3,
    cp2,
    mix3,
    sum3,
    acc,
    image,
    rows_ref,
    plane_buf,
    ring_buf,
    tr_sem,
    in_sem,
    halo_send,
    halo_recv,
    plane_send,
    plane_recv,
    ring_send,
    ring_recv,
    far_sem,
):
    n_vec, n_loc, coef, sph = basis_hbm.shape
    kinds = trans_hbm.shape[0]
    s_kinds = tmat_hbm.shape[0]
    slots = nbr_block_hbm.shape[1]
    most = n_vec + 1
    chunks = chunk_rows(coef)
    n_ring = n_blk // PLANE
    window = 3 * n_loc

    me = lax.axis_index("blk")
    z = me // PLANE
    q = me % PLANE
    left, right = me - 1, me + 1
    has_left, has_right = me > 0, me < n_blk - 1
    far_left = jnp.logical_and(q == 0, has_left)
    far_right = jnp.logical_and(q == PLANE - 1, has_right)

    own = pltpu.make_async_copy(
        basis_hbm.at[n_vec - 1], wins.at[0, pl.ds(n_loc, n_loc)], in_sem.at[0]
    )
    own.start()
    barrier = pltpu.get_barrier_semaphore()

    def signal(sem, target):
        pl.semaphore_signal(sem, inc=1, device_id={"blk": target}, device_id_type=MESH)

    def plane_peer(d):
        return z * PLANE + (q + d) % PLANE

    def ring_peer(d):
        return ((z + d) % n_ring) * PLANE + q

    for d in range(1, PLANE):
        signal(barrier, plane_peer(d))
    for d in (1, n_ring - 1):
        signal(barrier, ring_peer(d))

    @pl.when(far_left)
    def _():
        signal(barrier, left)

    @pl.when(far_right)
    def _():
        signal(barrier, right)

    reach = [1]
    while 2 * reach[-1] < n_ring:
        reach.append(2 * reach[-1])
    rounds = len(reach) - 1

    def far_signal(i):
        if i < rounds:
            for d in (reach[i], n_ring - reach[i]):
                signal(far_sem.at[i], ring_peer(d))

    def far_round(i):
        if i < rounds:
            pl.semaphore_wait(far_sem.at[i], 2)
            far_signal(i + 1)

    small = [
        pltpu.make_async_copy(src, dst, in_sem.at[4 + i])
        for i, (src, dst) in enumerate(
            (
                (nbr_block_hbm, nbr_block),
                (nbr_type_hbm, nbr_type),
                (nbr_count_hbm, nbr_count),
                (sphere_type_hbm, sphere_type),
                (table_hbm, table),
            )
        )
    ]
    for copy in small:
        copy.start()
    cp_copy = pltpu.make_async_copy(coup_hbm, cp32, in_sem.at[1])
    cp_copy.start()

    def trans_copy(r):
        lo, n = chunks[r]
        return pltpu.make_async_copy(
            trans_hbm.at[:, :, pl.ds(lo, n)], tr32.at[:, :, pl.ds(lo, n)], tr_sem.at[r]
        )

    for r in range(len(chunks)):
        trans_copy(r).start()
    tm_copy = pltpu.make_async_copy(tmat_hbm, tm32, in_sem.at[3])
    tm_copy.start()
    stack_copy = pltpu.make_async_copy(basis_hbm, stack, in_sem.at[2])
    stack_copy.start()

    def halo(step, side, r):
        lo, n = chunks[r]
        to = 0 if side == 0 else 2 * n_loc
        return pltpu.make_async_remote_copy(
            src_ref=wins.at[step, pl.ds(n_loc, n_loc), pl.ds(lo, n)],
            dst_ref=wins.at[step, pl.ds(to, n_loc), pl.ds(lo, n)],
            send_sem=halo_send.at[step, side, r],
            recv_sem=halo_recv.at[step, side, r],
            device_id={"blk": right if side == 0 else left},
            device_id_type=MESH,
        )

    def halo_start(step, r):
        @pl.when(has_right)
        def _():
            halo(step, 0, r).start()

        @pl.when(has_left)
        def _():
            halo(step, 1, r).start()

    def halo_wait(step, r):
        @pl.when(has_left)
        def _():
            halo(step, 0, r).wait_recv()

        @pl.when(has_right)
        def _():
            halo(step, 1, r).wait_recv()

    pl.semaphore_wait(
        barrier, PLANE + 1 + far_left.astype(jnp.int32) + far_right.astype(jnp.int32)
    )
    own.wait()
    for r in range(len(chunks)):
        halo_start(0, r)
    far_signal(0)

    @pl.when(jnp.logical_not(has_left))
    def _():
        wins[0, 0:n_loc] = jnp.zeros((n_loc, coef, sph), F32)
        wins[1, 0:n_loc] = jnp.zeros((n_loc, coef, sph), F32)

    @pl.when(jnp.logical_not(has_right))
    def _():
        wins[0, 2 * n_loc :] = jnp.zeros((n_loc, coef, sph), F32)
        wins[1, 2 * n_loc :] = jnp.zeros((n_loc, coef, sph), F32)

    for copy in small:
        copy.wait()
    first_block = me * n_loc
    slot_id = lax.broadcasted_iota(jnp.int32, (1, slots), 1)
    use_id = lax.broadcasted_iota(jnp.int32, (kinds * window, slots), 0)
    for b in range(n_loc):
        use = nbr_type[b : b + 1, :] * window + (nbr_block[b : b + 1, :] - first_block + n_loc)
        use = jnp.where(slot_id < nbr_count[b], use, -1)
        hits = jnp.sum(jnp.where(use_id == use, 1.0, 0.0), axis=1, keepdims=True)
        weights[b] = jnp.broadcast_to(hits, (kinds * window, LANES))

    rows_ref[...] = jnp.zeros_like(rows_ref)
    sum3[...] = jnp.zeros_like(sum3)
    mix3[0] = jnp.zeros_like(mix3[0])

    cp_copy.wait()

    def split_coup(t, carry):
        high, low = halves(cp32[t].T)
        cp2[t, 0, 0:sph] = high
        cp2[t, 0, sph:] = high
        cp2[t, 1, 0:sph] = low
        cp2[t, 1, sph:] = jnp.zeros_like(low)
        return carry

    lax.fori_loop(0, kinds, split_coup, 0, unroll=4)

    def split_left(x, n):
        if n < LANES:
            x = jnp.concatenate([x, jnp.zeros((coef, LANES - n), F32)], axis=1)
        return halves(x)

    def split_trans(r):
        lo, n = chunks[r]
        for t in range(kinds):
            high, low = split_left(tr32[t, :, lo : lo + n], n)
            tr3[r, 0, t] = high
            tr3[r, 1, t] = low

    def split_tmat():
        for t in range(s_kinds):
            for lo, n in chunks:
                high, low = split_left(tm32[t, :, lo : lo + n], n)
                tm3[t, 0, lo // LANES] = high
                tm3[t, 1, lo // LANES] = low

    depth = len(chunks) * LANES
    pairs = [(i, j) for i in range(n_vec) for j in range(i, n_vec)]

    def gram_step(g, sums):
        at = pl.multiple_of(g * 8, 8)
        sums = list(sums)
        for b in range(n_loc):
            vs = [stack[i, b, pl.ds(at, 8), :] for i in range(n_vec)]
            for c, (i, j) in enumerate(pairs):
                sums[c] = sums[c] + vs[i] * vs[j]
        return tuple(sums)

    def basis_pairs():
        gram = lax.fori_loop(
            0, coef // 8, gram_step, tuple(jnp.zeros((8, sph), F32) for _ in pairs)
        )
        for c, (i, j) in enumerate(pairs):
            at = lane_of[i, j]
            rows_ref[at : at + 1, :] = jnp.sum(gram[c], axis=0, keepdims=True)

    def three(left, right):
        high, low = right
        part = jnp.dot(left[0], high, preferred_element_type=F32)
        part += jnp.dot(left[1], high, preferred_element_type=F32)
        part += jnp.dot(left[0], low, preferred_element_type=F32)
        return part

    def wide_left(ref, lead, count, rows):
        return [
            jnp.concatenate([ref[(*lead, i, k, rows)] for k in range(count)], axis=1)
            for i in range(2)
        ]

    def wide_right(ref, lead):
        return [
            jnp.concatenate([ref[(*lead, i, b)] for b in range(n_loc)], axis=1)
            for i in range(2)
        ]

    half = coef // 2

    def product(r):
        for lo in (0, half):
            left = wide_left(tr3, (r,), kinds, slice(lo, lo + half))
            part = three(left, wide_right(mix3, (r % 2,)))
            if r == 0:
                acc[lo : lo + half] = part
            else:
                acc[lo : lo + half] += part

    def mix(step, r):
        lo, n = chunks[r]
        for t in range(kinds):
            blocks = []
            for b in range(n_loc):
                total = None
                for p in range(b, b + 2 * n_loc + 1):
                    c = t * window + p
                    term = weights[b, c : c + 1, :] * wins[step, p, lo : lo + n, :]
                    total = term if total is None else total + term
                blocks.append(total)
            high, low = halves(jnp.concatenate(blocks, axis=0))
            both = jnp.dot(
                jnp.concatenate([high, low], axis=1),
                jnp.concatenate([cp2[t, 0], cp2[t, 1]], axis=1),
                preferred_element_type=F32,
            )
            high, low = halves(both[:, :sph] + both[:, sph:])
            for i, part in enumerate((high, low)):
                for b in range(n_loc):
                    mix3[r % 2, i, b, t * LANES : t * LANES + n] = part[b * n : (b + 1) * n]

    def apply(step):
        last = len(chunks) - 1
        for r in range(len(chunks)):
            if step == 0 and r > 0:
                far_round(r - 1)
            halo_wait(step, r)
            mix(step, r)
            if r > 0:
                product(r - 1)

        @pl.when(me >= 0)
        def _():
            product(last)

        for lo, n in chunks:
            high, low = halves(acc[lo : lo + n, :])
            for b in range(n_loc):
                sum3[0, b, lo : lo + n] = high[:, b * sph : (b + 1) * sph]
                sum3[1, b, lo : lo + n] = low[:, b * sph : (b + 1) * sph]
        types = jnp.concatenate([sphere_type[b : b + 1, :] for b in range(n_loc)], axis=1)

        def scatter(i, carry):
            for t in (2 * i, 2 * i + 1):
                part = three(
                    wide_left(tm3, (t,), len(chunks), slice(None)), wide_right(sum3, ())
                )
                here = jnp.broadcast_to(types == t, part.shape)
                acc[...] = jnp.where(here, part, acc[...])
            return carry

        lax.fori_loop(0, s_kinds // 2, scatter, 0)
        for b in range(n_loc):
            image[b] = wins[step, n_loc + b] - acc[:, b * sph : (b + 1) * sph]

    GROUP = 40 if coef % 40 == 0 else 8

    def vector_rows(i, b, at):
        if i < n_vec:
            return stack[i, b, pl.ds(at, GROUP), :]
        return wins[1, n_loc + b, pl.ds(at, GROUP), :]

    def fold(x):
        return jnp.sum(x.reshape(GROUP // 8, 8, sph), axis=0)

    def dots(lefts, right_rows, extra):
        def body(g, sums):
            at = pl.multiple_of(g * GROUP, 8)
            sums = list(sums)
            for b in range(n_loc):
                w = right_rows(b, at)
                for c, i in enumerate(lefts):
                    sums[c] = sums[c] + fold(vector_rows(i, b, at) * w)
                if extra:
                    sums[-1] = sums[-1] + fold(w * w)
            return tuple(sums)

        zero = jnp.zeros((8, sph), F32)
        return lax.fori_loop(
            0, coef // GROUP, body, tuple(zero for _ in range(len(lefts) + int(extra)))
        )

    def lanes_of_rows():
        x = rows_ref[...]
        col = jnp.sum(x, axis=1, keepdims=True)
        row_id = lax.broadcasted_iota(jnp.int32, x.shape, 0)
        lane_id = lax.broadcasted_iota(jnp.int32, x.shape, 1)
        return jnp.sum(jnp.where(row_id == lane_id, col, 0.0), axis=0, keepdims=True)

    def plane_copy(step, d):
        return pltpu.make_async_remote_copy(
            src_ref=plane_buf.at[step, q],
            dst_ref=plane_buf.at[step, q],
            send_sem=plane_send.at[step, d],
            recv_sem=plane_recv.at[step, d],
            device_id={"blk": plane_peer(d)},
            device_id_type=MESH,
        )

    def ring_copy(step, d):
        return pltpu.make_async_remote_copy(
            src_ref=ring_buf.at[step, z],
            dst_ref=ring_buf.at[step, z],
            send_sem=ring_send.at[step, d],
            recv_sem=ring_recv.at[step, d],
            device_id={"blk": ring_peer(d)},
            device_id_type=MESH,
        )

    def all_reduce(step, x, meanwhile):
        plane_buf[step, q] = x
        for d in range(1, PLANE):
            plane_copy(step, d).start()
        for d in range(1, PLANE):
            plane_copy(step, d).wait_recv()
        ring_buf[step, z] = functools.reduce(
            jnp.add, [plane_buf[step, i] for i in range(PLANE)]
        )
        order = sorted(range(1, n_ring), key=lambda d: -min(d, n_ring - d))
        for d in order:
            ring_copy(step, d).start()
        meanwhile()
        for d in order:
            ring_copy(step, d).wait_recv()
        return functools.reduce(jnp.add, [ring_buf[step, i] for i in range(n_ring)])

    def reduced(step, n_used, meanwhile):
        sums = dots(range(n_used), lambda b, at: image[b, pl.ds(at, GROUP), :], True)
        for i in range(n_used):
            rows_ref[i : i + 1, :] = jnp.sum(sums[i], axis=0, keepdims=True)
        rows_ref[most : most + 1, :] = jnp.sum(sums[n_used], axis=0, keepdims=True)
        return all_reduce(step, lanes_of_rows(), meanwhile) * (1.0 / cells)

    def spread(row, i):
        return jnp.broadcast_to(row[:, i : i + 1], (1, LANES))

    def tall(row):
        return jnp.broadcast_to(row, (8, LANES))

    def vector8(i, b, at):
        if i < n_vec:
            return stack[i, b, pl.ds(at, 8), :]
        return wins[1, n_loc + b, pl.ds(at, 8), :]

    def combine(shares, scale, store, lo, n):
        def body(g, carry):
            at = pl.multiple_of(lo + g * 8, 8)
            for b in range(n_loc):
                u = image[b, pl.ds(at, 8), :]
                for i, share in enumerate(shares):
                    u = u - share * vector8(i, b, at)
                store(b, at, u * scale)
            return carry

        lax.fori_loop(0, n // 8, body, 0, unroll=4)

    lane = lax.broadcasted_iota(jnp.int32, (1, LANES), 1)

    for r in range(len(chunks)):
        trans_copy(r).wait()
        split_trans(r)
    tm_copy.wait()
    split_tmat()

    apply(0)
    stack_copy.wait()
    means = reduced(0, n_vec, basis_pairs)
    first_row = means
    size2 = spread(means, most) + 1e-6
    size = jnp.sqrt(size2)
    shares = [tall(spread(means, i)) for i in range(n_vec)]
    scale = tall(1.0 / size)

    def store_first(b, at, value):
        wins[1, n_loc + b, pl.ds(at, 8), :] = value

    for r, (lo, n) in enumerate(chunks):
        combine(shares, scale, store_first, lo, n)
        halo_start(1, r)

    def first_rows(b, at):
        return wins[1, n_loc + b, pl.ds(at, GROUP), :]

    new_pairs = dots(range(n_vec), first_rows, True)
    for i in range(most):
        at = lane_of[i, n_vec]
        rows_ref[at : at + 1, :] = jnp.sum(new_pairs[i], axis=0, keepdims=True)

    apply(1)
    means = reduced(1, most, lambda: None)
    norm1 = jnp.sqrt(size2 * spread(means, lane_of[n_vec, n_vec]) + 1e-6)
    ratio = size / norm1
    parts = [spread(means, i) for i in range(n_vec)]
    parts.append(ratio * ratio * spread(means, n_vec))

    def factor(which):
        out = jnp.where(which == most, 1.0, 0.0)
        for i in range(most):
            out = jnp.where(which == i, parts[i], out)
        return out

    share = means * table[2:3, :].astype(F32)
    share = share * factor(table[0:1, :]) * factor(table[1:2, :])
    squares = jnp.broadcast_to(jnp.sum(share, axis=1, keepdims=True), (1, LANES))
    norm2 = jnp.sqrt(ratio * ratio * jnp.maximum(squares, 0.0) + 1e-6)
    hess_ref[0:1, :] = jnp.where(lane == n_vec, norm1, first_row)
    second_row = ratio * jnp.where(lane == n_vec, ratio * means, means)
    hess_ref[1:2, :] = jnp.where(lane == most, norm2, second_row)

    grow = tall(ratio)

    def store_second(b, at, value):
        new_ref[1, b, pl.ds(at, 8), :] = value
        new_ref[0, b, pl.ds(at, 8), :] = vector8(n_vec, b, at) * grow

    combine([tall(p) for p in parts], tall(ratio / norm2), store_second, 0, coef)

    for step in range(2):
        for r in range(len(chunks)):

            @pl.when(has_right)
            def _():
                halo(step, 0, r).wait_send()

            @pl.when(has_left)
            def _():
                halo(step, 1, r).wait_send()

        for d in range(1, PLANE):
            plane_copy(step, d).wait_send()
        for d in range(1, n_ring):
            ring_copy(step, d).wait_send()


def finish(new_in, hess, new_out, first, second, sem):
    store = pltpu.make_async_copy(new_in, new_out, sem)
    store.start()
    first[...] = hess[0, : first.shape[0]]
    second[...] = hess[1, : second.shape[0]]
    store.wait()


def shards(n_blk, basis, nbr_block, nbr_type, nbr_count, sphere_type, trans, coup, tmat):
    n_vec, n_loc, coef, sph = basis.shape
    kinds, s_kinds = trans.shape[0], tmat.shape[0]
    chunks = chunk_rows(coef)
    n_ring = n_blk // PLANE
    table, lane_of, used = lane_tables(n_vec + 1)
    cells = float(n_blk * n_loc * coef * sph)
    hbm = pl.BlockSpec(memory_space=pltpu.HBM)
    vmem = pl.BlockSpec(memory_space=pltpu.VMEM)
    dma = pltpu.SemaphoreType.DMA
    wide = n_loc * sph
    in_hbm = functools.partial(pltpu.with_memory_space_constraint, memory_space=pltpu.HBM)
    new, hess = pl.pallas_call(
        functools.partial(kernel, n_blk, cells, lane_of),
        out_shape=(
            jax.ShapeDtypeStruct((2, n_loc, coef, sph), F32),
            jax.ShapeDtypeStruct((8, LANES), F32),
        ),
        in_specs=[hbm] * 9,
        out_specs=(vmem, vmem),
        scratch_shapes=[
            pltpu.VMEM(nbr_block.shape, jnp.int32),
            pltpu.VMEM(nbr_type.shape, jnp.int32),
            pltpu.SMEM(nbr_count.shape, jnp.int32),
            pltpu.VMEM(sphere_type.shape, jnp.int32),
            pltpu.VMEM(table.shape, jnp.int32),
            pltpu.VMEM((n_loc, kinds * 3 * n_loc, LANES), F32),
            pltpu.VMEM((2, 3 * n_loc, coef, sph), F32),
            pltpu.VMEM((n_vec, n_loc, coef, sph), F32),
            pltpu.VMEM(trans.shape, F32),
            pltpu.VMEM(tmat.shape, F32),
            pltpu.VMEM(coup.shape, F32),
            pltpu.VMEM((len(chunks), 2, kinds, coef, LANES), BF16),
            pltpu.VMEM((s_kinds, 2, len(chunks), coef, LANES), BF16),
            pltpu.VMEM((kinds, 2, 2 * sph, sph), BF16),
            pltpu.VMEM((2, 2, n_loc, kinds * LANES, sph), BF16),
            pltpu.VMEM((2, n_loc, len(chunks) * LANES, sph), BF16),
            pltpu.VMEM((coef, wide), F32),
            pltpu.VMEM((n_loc, coef, sph), F32),
            pltpu.VMEM(((used + 7) // 8 * 8, LANES), F32),
            pltpu.VMEM((2, PLANE, 1, LANES), F32),
            pltpu.VMEM((2, n_ring, 1, LANES), F32),
            dma((len(chunks),)),
            dma((9,)),
            dma((2, 2, len(chunks))),
            dma((2, 2, len(chunks))),
            dma((2, PLANE)),
            dma((2, PLANE)),
            dma((2, n_ring)),
            dma((2, n_ring)),
            pltpu.SemaphoreType.REGULAR((max(1, n_ring.bit_length()),)),
        ],
        compiler_params=pltpu.CompilerParams(
            collective_id=0, has_side_effects=True, vmem_limit_bytes=52 * 1024 * 1024
        ),
    )(
        *map(
            in_hbm,
            (
                basis,
                nbr_block,
                nbr_type,
                nbr_count,
                sphere_type,
                jnp.asarray(table),
                trans,
                coup,
                tmat,
            ),
        )
    )
    return pl.pallas_call(
        finish,
        out_shape=(
            jax.ShapeDtypeStruct(new.shape, F32),
            jax.ShapeDtypeStruct((n_vec + 1,), F32),
            jax.ShapeDtypeStruct((n_vec + 2,), F32),
        ),
        in_specs=[vmem, vmem],
        out_specs=(hbm, vmem, vmem),
        scratch_shapes=[dma],
        compiler_params=pltpu.CompilerParams(vmem_limit_bytes=4 * 1024 * 1024),
    )(new, hess)


def solution(mesh):
    return jax.shard_map(
        functools.partial(shards, mesh.shape["blk"]),
        mesh=mesh,
        in_specs=(
            P(None, GB, None, None),
            P(GB, None),
            P(GB, None),
            P(GB),
            P(GB, None),
            P(),
            P(),
            P(),
        ),
        out_specs=(P(None, GB, None, None), P("groups"), P("groups")),
        check_vma=False,
    )
```

```python
import functools

import jax
import jax.numpy as jnp
import numpy as np
from jax import lax
from jax.experimental import pallas as pl
from jax.experimental.pallas import tpu as pltpu
from jax.sharding import PartitionSpec as P

GB = ("groups", "blk")
PLANE = 8
LANES = 128
F32 = jnp.float32
BF16 = jnp.bfloat16
MESH = pl.DeviceIdType.MESH


def chunk_rows(coef):
    parts = [(c, min(LANES, coef - c)) for c in range(0, coef, LANES)]
    return parts[-1:] + parts[:-1]


def lane_tables(most):
    one = most
    table = np.zeros((8, LANES), np.int32)
    table[0:2, :] = most + 1
    lane_of = {}
    for i in range(most):
        table[0:3, i] = (i, one, -2)
    table[0:3, most] = (one, one, 1)
    at = most + 1
    for i in range(most):
        for j in range(i, most):
            table[0:3, at] = (i, j, 1 if i == j else 2)
            lane_of[i, j] = at
            at += 1
    return table, lane_of, at


def halves(x):
    high = x.astype(BF16)
    return high, (x - high.astype(F32)).astype(BF16)


def kernel(
    n_blk,
    cells,
    lane_of,
    basis_hbm,
    nbr_block_hbm,
    nbr_type_hbm,
    nbr_count_hbm,
    sphere_type_hbm,
    table_hbm,
    trans_hbm,
    coup_hbm,
    tmat_hbm,
    new_ref,
    hess_ref,
    nbr_block,
    nbr_type,
    nbr_count,
    sphere_type,
    table,
    weights,
    wins,
    stack,
    tr32,
    tm32,
    cp32,
    tr3,
    tm3,
    cp2,
    mix3,
    sum3,
    acc,
    image,
    rows_ref,
    plane_buf,
    ring_buf,
    tr_sem,
    in_sem,
    halo_send,
    halo_recv,
    plane_send,
    plane_recv,
    ring_send,
    ring_recv,
    far_sem,
):
    n_vec, n_loc, coef, sph = basis_hbm.shape
    kinds = trans_hbm.shape[0]
    s_kinds = tmat_hbm.shape[0]
    slots = nbr_block_hbm.shape[1]
    most = n_vec + 1
    chunks = chunk_rows(coef)
    n_ring = n_blk // PLANE
    window = 3 * n_loc

    me = lax.axis_index("blk")
    z = me // PLANE
    q = me % PLANE
    left, right = me - 1, me + 1
    has_left, has_right = me > 0, me < n_blk - 1
    far_left = jnp.logical_and(q == 0, has_left)
    far_right = jnp.logical_and(q == PLANE - 1, has_right)

    own = pltpu.make_async_copy(
        basis_hbm.at[n_vec - 1], wins.at[0, pl.ds(n_loc, n_loc)], in_sem.at[0]
    )
    own.start()
    barrier = pltpu.get_barrier_semaphore()

    def signal(sem, target):
        pl.semaphore_signal(sem, inc=1, device_id={"blk": target}, device_id_type=MESH)

    def plane_peer(d):
        return z * PLANE + (q + d) % PLANE

    def ring_peer(d):
        return ((z + d) % n_ring) * PLANE + q

    for d in range(1, PLANE):
        signal(barrier, plane_peer(d))
    for d in (1, n_ring - 1):
        signal(barrier, ring_peer(d))

    @pl.when(far_left)
    def _():
        signal(barrier, left)

    @pl.when(far_right)
    def _():
        signal(barrier, right)

    reach = [1]
    while 2 * reach[-1] < n_ring:
        reach.append(2 * reach[-1])
    rounds = len(reach) - 1

    def far_signal(i):
        if i < rounds:
            for d in (reach[i], n_ring - reach[i]):
                signal(far_sem.at[i], ring_peer(d))

    def far_round(i):
        if i < rounds:
            pl.semaphore_wait(far_sem.at[i], 2)
            far_signal(i + 1)

    small = [
        pltpu.make_async_copy(src, dst, in_sem.at[4 + i])
        for i, (src, dst) in enumerate(
            (
                (nbr_block_hbm, nbr_block),
                (nbr_type_hbm, nbr_type),
                (nbr_count_hbm, nbr_count),
                (sphere_type_hbm, sphere_type),
                (table_hbm, table),
            )
        )
    ]
    for copy in small:
        copy.start()
    cp_copy = pltpu.make_async_copy(coup_hbm, cp32, in_sem.at[1])
    cp_copy.start()

    def trans_copy(r):
        lo, n = chunks[r]
        return pltpu.make_async_copy(
            trans_hbm.at[:, :, pl.ds(lo, n)], tr32.at[:, :, pl.ds(lo, n)], tr_sem.at[r]
        )

    for r in range(len(chunks)):
        trans_copy(r).start()
    tm_copy = pltpu.make_async_copy(tmat_hbm, tm32, in_sem.at[3])
    tm_copy.start()
    stack_copy = pltpu.make_async_copy(basis_hbm, stack, in_sem.at[2])
    stack_copy.start()

    def halo(step, side, r):
        lo, n = chunks[r]
        to = 0 if side == 0 else 2 * n_loc
        return pltpu.make_async_remote_copy(
            src_ref=wins.at[step, pl.ds(n_loc, n_loc), pl.ds(lo, n)],
            dst_ref=wins.at[step, pl.ds(to, n_loc), pl.ds(lo, n)],
            send_sem=halo_send.at[step, side, r],
            recv_sem=halo_recv.at[step, side, r],
            device_id={"blk": right if side == 0 else left},
            device_id_type=MESH,
        )

    def halo_start(step, r):
        @pl.when(has_right)
        def _():
            halo(step, 0, r).start()

        @pl.when(has_left)
        def _():
            halo(step, 1, r).start()

    def halo_wait(step, r):
        @pl.when(has_left)
        def _():
            halo(step, 0, r).wait_recv()

        @pl.when(has_right)
        def _():
            halo(step, 1, r).wait_recv()

    @pl.when(jnp.logical_not(has_left))
    def _():
        wins[0, 0:n_loc] = jnp.zeros((n_loc, coef, sph), F32)
        wins[1, 0:n_loc] = jnp.zeros((n_loc, coef, sph), F32)

    @pl.when(jnp.logical_not(has_right))
    def _():
        wins[0, 2 * n_loc :] = jnp.zeros((n_loc, coef, sph), F32)
        wins[1, 2 * n_loc :] = jnp.zeros((n_loc, coef, sph), F32)

    for copy in small:
        copy.wait()
    first_block = me * n_loc
    slot_id = lax.broadcasted_iota(jnp.int32, (1, slots), 1)
    use_id = lax.broadcasted_iota(jnp.int32, (kinds * window, slots), 0)
    for b in range(n_loc):
        use = nbr_type[b : b + 1, :] * window + (nbr_block[b : b + 1, :] - first_block + n_loc)
        use = jnp.where(slot_id < nbr_count[b], use, -1)
        hits = jnp.sum(jnp.where(use_id == use, 1.0, 0.0), axis=1, keepdims=True)
        weights[b] = jnp.broadcast_to(hits, (kinds * window, LANES))

    rows_ref[...] = jnp.zeros_like(rows_ref)
    sum3[...] = jnp.zeros_like(sum3)
    mix3[0] = jnp.zeros_like(mix3[0])

    cp_copy.wait()

    def split_coup(t, carry):
        high, low = halves(cp32[t].T)
        cp2[t, 0, 0:sph] = high
        cp2[t, 0, sph:] = high
        cp2[t, 1, 0:sph] = low
        cp2[t, 1, sph:] = jnp.zeros_like(low)
        return carry

    lax.fori_loop(0, kinds, split_coup, 0, unroll=4)

    pl.semaphore_wait(
        barrier, PLANE + 1 + far_left.astype(jnp.int32) + far_right.astype(jnp.int32)
    )
    own.wait()
    for r in range(len(chunks)):
        halo_start(0, r)
    far_signal(0)

    def split_left(x, n):
        if n < LANES:
            x = jnp.concatenate([x, jnp.zeros((coef, LANES - n), F32)], axis=1)
        return halves(x)

    def split_trans(r):
        lo, n = chunks[r]
        for t in range(kinds):
            high, low = split_left(tr32[t, :, lo : lo + n], n)
            tr3[r, 0, t] = high
            tr3[r, 1, t] = low

    def split_tmat():
        for t in range(s_kinds):
            for lo, n in chunks:
                high, low = split_left(tm32[t, :, lo : lo + n], n)
                tm3[t, 0, lo // LANES] = high
                tm3[t, 1, lo // LANES] = low

    depth = len(chunks) * LANES
    pairs = [(i, j) for i in range(n_vec) for j in range(i, n_vec)]

    def gram_step(g, sums):
        at = pl.multiple_of(g * 8, 8)
        sums = list(sums)
        for b in range(n_loc):
            vs = [stack[i, b, pl.ds(at, 8), :] for i in range(n_vec)]
            for c, (i, j) in enumerate(pairs):
                sums[c] = sums[c] + vs[i] * vs[j]
        return tuple(sums)

    def basis_pairs():
        gram = lax.fori_loop(
            0, coef // 8, gram_step, tuple(jnp.zeros((8, sph), F32) for _ in pairs)
        )
        for c, (i, j) in enumerate(pairs):
            at = lane_of[i, j]
            rows_ref[at : at + 1, :] = jnp.sum(gram[c], axis=0, keepdims=True)

    def three(left, right):
        high, low = right
        part = jnp.dot(left[0], high, preferred_element_type=F32)
        part += jnp.dot(left[1], high, preferred_element_type=F32)
        part += jnp.dot(left[0], low, preferred_element_type=F32)
        return part

    def wide_left(ref, lead, count, rows):
        return [
            jnp.concatenate([ref[(*lead, i, k, rows)] for k in range(count)], axis=1)
            for i in range(2)
        ]

    def wide_right(ref, lead):
        return [
            jnp.concatenate([ref[(*lead, i, b)] for b in range(n_loc)], axis=1)
            for i in range(2)
        ]

    half = coef // 2

    def product(r):
        for lo in (0, half):
            left = wide_left(tr3, (r,), kinds, slice(lo, lo + half))
            part = three(left, wide_right(mix3, (r % 2,)))
            if r == 0:
                acc[lo : lo + half] = part
            else:
                acc[lo : lo + half] += part

    def mix(step, r):
        lo, n = chunks[r]
        for t in range(kinds):
            blocks = []
            for b in range(n_loc):
                total = None
                for p in range(b, b + 2 * n_loc + 1):
                    c = t * window + p
                    term = weights[b, c : c + 1, :] * wins[step, p, lo : lo + n, :]
                    total = term if total is None else total + term
                blocks.append(total)
            high, low = halves(jnp.concatenate(blocks, axis=0))
            both = jnp.dot(
                jnp.concatenate([high, low], axis=1),
                jnp.concatenate([cp2[t, 0], cp2[t, 1]], axis=1),
                preferred_element_type=F32,
            )
            high, low = halves(both[:, :sph] + both[:, sph:])
            for i, part in enumerate((high, low)):
                for b in range(n_loc):
                    mix3[r % 2, i, b, t * LANES : t * LANES + n] = part[b * n : (b + 1) * n]

    def apply(step):
        last = len(chunks) - 1
        for r in range(len(chunks)):
            halo_wait(step, r)
            mix(step, r)
            if r > 0:
                product(r - 1)

        @pl.when(me >= 0)
        def _():
            product(last)

        for lo, n in chunks:
            high, low = halves(acc[lo : lo + n, :])
            for b in range(n_loc):
                sum3[0, b, lo : lo + n] = high[:, b * sph : (b + 1) * sph]
                sum3[1, b, lo : lo + n] = low[:, b * sph : (b + 1) * sph]
        types = jnp.concatenate([sphere_type[b : b + 1, :] for b in range(n_loc)], axis=1)

        def scatter(i, carry):
            for t in (2 * i, 2 * i + 1):
                part = three(
                    wide_left(tm3, (t,), len(chunks), slice(None)), wide_right(sum3, ())
                )
                here = jnp.broadcast_to(types == t, part.shape)
                acc[...] = jnp.where(here, part, acc[...])
            return carry

        if step == 0:
            for i in range(1, rounds - 1):
                far_round(i)
        lax.fori_loop(0, s_kinds // 2, scatter, 0)
        for b in range(n_loc):
            image[b] = wins[step, n_loc + b] - acc[:, b * sph : (b + 1) * sph]

    GROUP = 40 if coef % 40 == 0 else 8

    def vector_rows(i, b, at):
        if i < n_vec:
            return stack[i, b, pl.ds(at, GROUP), :]
        return wins[1, n_loc + b, pl.ds(at, GROUP), :]

    def fold(x):
        return jnp.sum(x.reshape(GROUP // 8, 8, sph), axis=0)

    def dots(lefts, right_rows, extra):
        def body(g, sums):
            at = pl.multiple_of(g * GROUP, 8)
            sums = list(sums)
            for b in range(n_loc):
                w = right_rows(b, at)
                for c, i in enumerate(lefts):
                    sums[c] = sums[c] + fold(vector_rows(i, b, at) * w)
                if extra:
                    sums[-1] = sums[-1] + fold(w * w)
            return tuple(sums)

        zero = jnp.zeros((8, sph), F32)
        return lax.fori_loop(
            0, coef // GROUP, body, tuple(zero for _ in range(len(lefts) + int(extra)))
        )

    def lanes_of_rows():
        x = rows_ref[...]
        col = jnp.sum(x, axis=1, keepdims=True)
        row_id = lax.broadcasted_iota(jnp.int32, x.shape, 0)
        lane_id = lax.broadcasted_iota(jnp.int32, x.shape, 1)
        return jnp.sum(jnp.where(row_id == lane_id, col, 0.0), axis=0, keepdims=True)

    def plane_copy(step, d):
        return pltpu.make_async_remote_copy(
            src_ref=plane_buf.at[step, q],
            dst_ref=plane_buf.at[step, q],
            send_sem=plane_send.at[step, d],
            recv_sem=plane_recv.at[step, d],
            device_id={"blk": plane_peer(d)},
            device_id_type=MESH,
        )

    def ring_copy(step, d):
        return pltpu.make_async_remote_copy(
            src_ref=ring_buf.at[step, z],
            dst_ref=ring_buf.at[step, z],
            send_sem=ring_send.at[step, d],
            recv_sem=ring_recv.at[step, d],
            device_id={"blk": ring_peer(d)},
            device_id_type=MESH,
        )

    def all_reduce(step, x, meanwhile):
        plane_buf[step, q] = x
        for d in range(1, PLANE):
            plane_copy(step, d).start()
        for d in range(1, PLANE):
            plane_copy(step, d).wait_recv()
        ring_buf[step, z] = functools.reduce(
            jnp.add, [plane_buf[step, i] for i in range(PLANE)]
        )
        if step == 0:
            for i in range(max(1, rounds - 1), rounds):
                far_round(i)
        order = sorted(range(1, n_ring), key=lambda d: -min(d, n_ring - d))
        for d in order:
            ring_copy(step, d).start()
        meanwhile()
        for d in order:
            ring_copy(step, d).wait_recv()
        return functools.reduce(jnp.add, [ring_buf[step, i] for i in range(n_ring)])

    def reduced(step, n_used, meanwhile):
        sums = dots(range(n_used), lambda b, at: image[b, pl.ds(at, GROUP), :], True)
        for i in range(n_used):
            rows_ref[i : i + 1, :] = jnp.sum(sums[i], axis=0, keepdims=True)
        rows_ref[most : most + 1, :] = jnp.sum(sums[n_used], axis=0, keepdims=True)
        return all_reduce(step, lanes_of_rows(), meanwhile) * (1.0 / cells)

    def spread(row, i):
        return jnp.broadcast_to(row[:, i : i + 1], (1, LANES))

    def tall(row):
        return jnp.broadcast_to(row, (8, LANES))

    def vector8(i, b, at):
        if i < n_vec:
            return stack[i, b, pl.ds(at, 8), :]
        return wins[1, n_loc + b, pl.ds(at, 8), :]

    def combine(shares, scale, store, lo, n):
        def body(g, carry):
            at = pl.multiple_of(lo + g * 8, 8)
            for b in range(n_loc):
                u = image[b, pl.ds(at, 8), :]
                for i, share in enumerate(shares):
                    u = u - share * vector8(i, b, at)
                store(b, at, u * scale)
            return carry

        lax.fori_loop(0, n // 8, body, 0, unroll=4)

    lane = lax.broadcasted_iota(jnp.int32, (1, LANES), 1)

    for r in range(len(chunks)):
        trans_copy(r).wait()
        split_trans(r)
    tm_copy.wait()
    split_tmat()
    far_round(0)

    apply(0)
    stack_copy.wait()
    means = reduced(0, n_vec, basis_pairs)
    first_row = means
    size2 = spread(means, most) + 1e-6
    size = jnp.sqrt(size2)
    shares = [tall(spread(means, i)) for i in range(n_vec)]
    scale = tall(1.0 / size)

    def store_first(b, at, value):
        wins[1, n_loc + b, pl.ds(at, 8), :] = value

    for r, (lo, n) in enumerate(chunks):
        combine(shares, scale, store_first, lo, n)
        halo_start(1, r)

    def first_rows(b, at):
        return wins[1, n_loc + b, pl.ds(at, GROUP), :]

    new_pairs = dots(range(n_vec), first_rows, True)
    for i in range(most):
        at = lane_of[i, n_vec]
        rows_ref[at : at + 1, :] = jnp.sum(new_pairs[i], axis=0, keepdims=True)

    apply(1)
    means = reduced(1, most, lambda: None)
    norm1 = jnp.sqrt(size2 * spread(means, lane_of[n_vec, n_vec]) + 1e-6)
    ratio = size / norm1
    parts = [spread(means, i) for i in range(n_vec)]
    parts.append(ratio * ratio * spread(means, n_vec))

    def factor(which):
        out = jnp.where(which == most, 1.0, 0.0)
        for i in range(most):
            out = jnp.where(which == i, parts[i], out)
        return out

    share = means * table[2:3, :].astype(F32)
    share = share * factor(table[0:1, :]) * factor(table[1:2, :])
    squares = jnp.broadcast_to(jnp.sum(share, axis=1, keepdims=True), (1, LANES))
    norm2 = jnp.sqrt(ratio * ratio * jnp.maximum(squares, 0.0) + 1e-6)
    hess_ref[0:1, :] = jnp.where(lane == n_vec, norm1, first_row)
    second_row = ratio * jnp.where(lane == n_vec, ratio * means, means)
    hess_ref[1:2, :] = jnp.where(lane == most, norm2, second_row)

    grow = tall(ratio)

    def store_second(b, at, value):
        new_ref[1, b, pl.ds(at, 8), :] = value
        new_ref[0, b, pl.ds(at, 8), :] = vector8(n_vec, b, at) * grow

    combine([tall(p) for p in parts], tall(ratio / norm2), store_second, 0, coef)

    for step in range(2):
        for r in range(len(chunks)):

            @pl.when(has_right)
            def _():
                halo(step, 0, r).wait_send()

            @pl.when(has_left)
            def _():
                halo(step, 1, r).wait_send()

        for d in range(1, PLANE):
            plane_copy(step, d).wait_send()
        for d in range(1, n_ring):
            ring_copy(step, d).wait_send()


def finish(new_in, hess, new_out, first, second, sem):
    store = pltpu.make_async_copy(new_in, new_out, sem)
    store.start()
    first[...] = hess[0, : first.shape[0]]
    second[...] = hess[1, : second.shape[0]]
    store.wait()


def shards(n_blk, basis, nbr_block, nbr_type, nbr_count, sphere_type, trans, coup, tmat):
    n_vec, n_loc, coef, sph = basis.shape
    kinds, s_kinds = trans.shape[0], tmat.shape[0]
    chunks = chunk_rows(coef)
    n_ring = n_blk // PLANE
    table, lane_of, used = lane_tables(n_vec + 1)
    cells = float(n_blk * n_loc * coef * sph)
    hbm = pl.BlockSpec(memory_space=pltpu.HBM)
    vmem = pl.BlockSpec(memory_space=pltpu.VMEM)
    dma = pltpu.SemaphoreType.DMA
    wide = n_loc * sph
    in_hbm = functools.partial(pltpu.with_memory_space_constraint, memory_space=pltpu.HBM)
    new, hess = pl.pallas_call(
        functools.partial(kernel, n_blk, cells, lane_of),
        out_shape=(
            jax.ShapeDtypeStruct((2, n_loc, coef, sph), F32),
            jax.ShapeDtypeStruct((8, LANES), F32),
        ),
        in_specs=[hbm] * 9,
        out_specs=(vmem, vmem),
        scratch_shapes=[
            pltpu.VMEM(nbr_block.shape, jnp.int32),
            pltpu.VMEM(nbr_type.shape, jnp.int32),
            pltpu.SMEM(nbr_count.shape, jnp.int32),
            pltpu.VMEM(sphere_type.shape, jnp.int32),
            pltpu.VMEM(table.shape, jnp.int32),
            pltpu.VMEM((n_loc, kinds * 3 * n_loc, LANES), F32),
            pltpu.VMEM((2, 3 * n_loc, coef, sph), F32),
            pltpu.VMEM((n_vec, n_loc, coef, sph), F32),
            pltpu.VMEM(trans.shape, F32),
            pltpu.VMEM(tmat.shape, F32),
            pltpu.VMEM(coup.shape, F32),
            pltpu.VMEM((len(chunks), 2, kinds, coef, LANES), BF16),
            pltpu.VMEM((s_kinds, 2, len(chunks), coef, LANES), BF16),
            pltpu.VMEM((kinds, 2, 2 * sph, sph), BF16),
            pltpu.VMEM((2, 2, n_loc, kinds * LANES, sph), BF16),
            pltpu.VMEM((2, n_loc, len(chunks) * LANES, sph), BF16),
            pltpu.VMEM((coef, wide), F32),
            pltpu.VMEM((n_loc, coef, sph), F32),
            pltpu.VMEM(((used + 7) // 8 * 8, LANES), F32),
            pltpu.VMEM((2, PLANE, 1, LANES), F32),
            pltpu.VMEM((2, n_ring, 1, LANES), F32),
            dma((len(chunks),)),
            dma((9,)),
            dma((2, 2, len(chunks))),
            dma((2, 2, len(chunks))),
            dma((2, PLANE)),
            dma((2, PLANE)),
            dma((2, n_ring)),
            dma((2, n_ring)),
            pltpu.SemaphoreType.REGULAR((max(1, n_ring.bit_length()),)),
        ],
        compiler_params=pltpu.CompilerParams(
            collective_id=0, has_side_effects=True, vmem_limit_bytes=52 * 1024 * 1024
        ),
    )(
        *map(
            in_hbm,
            (
                basis,
                nbr_block,
                nbr_type,
                nbr_count,
                sphere_type,
                jnp.asarray(table),
                trans,
                coup,
                tmat,
            ),
        )
    )
    return pl.pallas_call(
        finish,
        out_shape=(
            jax.ShapeDtypeStruct(new.shape, F32),
            jax.ShapeDtypeStruct((n_vec + 1,), F32),
            jax.ShapeDtypeStruct((n_vec + 2,), F32),
        ),
        in_specs=[vmem, vmem],
        out_specs=(hbm, vmem, vmem),
        scratch_shapes=[dma],
        compiler_params=pltpu.CompilerParams(vmem_limit_bytes=4 * 1024 * 1024),
    )(new, hess)


def solution(mesh):
    return jax.shard_map(
        functools.partial(shards, mesh.shape["blk"]),
        mesh=mesh,
        in_specs=(
            P(None, GB, None, None),
            P(GB, None),
            P(GB, None),
            P(GB),
            P(GB, None),
            P(),
            P(),
            P(),
        ),
        out_specs=(P(None, GB, None, None), P("groups"), P("groups")),
        check_vma=False,
    )
```
